128 devices in a mesh: grp: 4 (over z_lo, core), tile: 32 (over x, z_hi, y).
Axes of the slice: x: 4, y: 4, z: 4 (z_hi: 2, z_lo: 2; z = z_hi * 2 + z_lo), core: 2. Of those that a mesh axis runs over, the one named last changes fastest.
Arguments:
- amplitudes: bfloat16 [160, 4, 983040], P(None, None, ('grp', 'tile')), may hold values from -6 to 6
- w_vvvo: bfloat16 [1024, 983040], P(None, ('grp', 'tile')), may hold values from -0.0234375 to 0.0234375
- pair_mask: int32 [4096], P(('grp', 'tile')), may hold values from 0 to 1, as said below
- owner_map: int32 [32], replicated, may hold values from 0 to 31, each once
Outputs:
- sigma_one: float32 [160, 4, 1024], P('tile', None, 'grp')
The draws below stay inside these ranges and needn't reach their ends.
Inputs may be any that keep to these rules, and one draw needn't show every extreme that they name: `pair_mask`: in each aligned block of 32 pairs at most 24 are 1 and at least one is; some block has exactly 24 and some block exactly one. `owner_map`: a permutation of the row blocks.
All inputs are finite; a program needn't handle non-finite values.
Results may differ from the reference program's by a relative error of at most 0.0003.
Values sent between devices are 32-bit elements; how exact they have to be, the bound alone decides.
A program may use at most 128 MiB of HBM per device.

```python
import jax
import jax.numpy as jnp
from jax import lax

V = 1024
O = 240
NR = 4
IROW = 5
PAIR_DEV = 32
LIVE_DEV = 24
I = 160
PAIRS = 4096
N_TILE = 32


def draw_pair_mask(key, part):
    groups = PAIRS // PAIR_DEV
    base = jax.random.fold_in(key, 11)
    key_count, key_full, key_perm = jax.random.split(base, 3)
    counts = jax.random.randint(key_count, (groups,), 1, LIVE_DEV + 1)
    full_group = jax.random.randint(key_full, (), 0, groups)
    sparse_group = (full_group + 1) % groups
    counts = jnp.where(jnp.arange(groups) == full_group, LIVE_DEV, counts)
    counts = jnp.where(jnp.arange(groups) == sparse_group, 1, counts)
    order_ranks = jax.vmap(lambda subkey: jax.random.permutation(subkey, PAIR_DEV))(jax.random.split(key_perm, groups))
    return (order_ranks < counts[:, None]).astype(jnp.int32).reshape(PAIRS)


def with_spikes(result, rng, source, target, blocks, factor):
    owner, partner = [(jnp.arange(result.shape[axis_at]) // (result.shape[axis_at] // blocks)).reshape([-1 if axis == axis_at else 1 for axis in range(result.ndim)]) for axis_at in (source, target)]
    chosen = jax.random.permutation(rng, blocks)[partner]
    strong = (owner == chosen) | (owner == (partner + blocks // 2) % blocks)
    return jnp.where(strong, factor * result, result)


def block_levels(key, dims, shards, low, top_value):
    loudness = 1.0
    for axis_at, parts in shards:
        draws = jax.random.uniform(jax.random.fold_in(jax.random.fold_in(key, 6), axis_at), (parts,), jnp.float32, low / len(shards), top_value / len(shards))
        loudness = loudness * jnp.repeat(jnp.exp(draws), dims[axis_at] // parts).reshape((-1,) + (1,) * (len(dims) - 1 - axis_at))
    return loudness


def centred(own_key, dims, deviation, bound, shards=(), held_as=jnp.bfloat16):
    loudness = block_levels(own_key, dims, shards, -0.22, 0.18) if shards else 1.0
    drawn = jax.random.normal(own_key, dims, jnp.float32) * deviation * loudness
    return jnp.minimum(jnp.maximum(drawn, -bound), bound).astype(held_as)


def noise_with(key, extent, spread, bound, pieces, heavy, held_as=jnp.bfloat16):
    array = spread * jax.random.normal(key, extent, jnp.float32)
    if pieces:
        array = array * block_levels(key, extent, pieces, -0.22, 0.18)
    return jnp.clip(with_spikes(array, jax.random.fold_in(key, 3), *heavy), -bound, bound).astype(held_as)


def setup_inputs(seed: int = 0) -> dict:
    splits = jax.random.split(jax.random.key(seed), 5)
    return {
        "amplitudes": centred(splits[0], (I, NR, PAIRS * O), 1.0, 6.0, ((2, 128),)),
        "w_vvvo": noise_with(splits[1], (V, PAIRS * O), (PAIRS * O) ** -0.5, 0.0234375, ((1, 128),), (1, 0, 128, 5.5)),
        "pair_mask": draw_pair_mask(jax.random.fold_in(splits[4], 71), 0),
        "owner_map": jax.random.permutation(splits[3], N_TILE).astype(jnp.int32),
    }


def reference(amplitudes, w_vvvo, pair_mask, owner_map):
    block_cols = PAIR_DEV * O
    block_total = PAIRS // PAIR_DEV

    def add_block(running, index):
        offset = (index * block_cols).astype(jnp.int32)
        amp_block = lax.dynamic_slice_in_dim(amplitudes, offset, block_cols, 2).astype(jnp.float32)
        mask_part = lax.dynamic_slice_in_dim(pair_mask, (index * PAIR_DEV).astype(jnp.int32), PAIR_DEV, 0)
        mask_cols = jnp.repeat(mask_part.astype(jnp.float32), O)
        w_block = lax.dynamic_slice_in_dim(w_vvvo, offset, block_cols, 1).astype(jnp.float32)
        masked = amp_block * mask_cols
        return running + jnp.einsum("irk,ak->ira", masked, w_block, precision=lax.Precision.HIGHEST), None

    start_value = jnp.zeros((I, NR, V), jnp.float32)
    full_sigma, _ = lax.scan(add_block, start_value, jnp.arange(block_total, dtype=jnp.int32))
    blocked = full_sigma.reshape(N_TILE, IROW, NR, V)
    ordered = jnp.take(blocked, owner_map.astype(jnp.int32), axis=0)
    return ordered.reshape(I, NR, V)
```

```python
import jax
import jax.numpy as jnp
from jax import lax
from jax.experimental import pallas as pl
from jax.experimental.pallas import tpu as pltpu
from jax.sharding import PartitionSpec as P

MESH = pl.DeviceIdType.MESH
F32 = jnp.float32
BF16 = jnp.bfloat16

NK = 15
KC = 512
OCC = 240
AHEAD = 4
ROWS = (8, 8, 4)
BASE = (0, 32, 64)
LANES = 128


def kernel(
    pm, om, a_hbm, w_hbm, out, a_raw, a2, wb, sib0, sib1, own0, own1, prt0, prt1, s0, s1, s2, r10, r11, r12,
    r20, r21, r22, r30, r31, r32, t10, t11, t12, t20, t21, t22,
    sem_a, sem_w, dsend, drecv, ssend, srecv,
):
    grp = lax.axis_index("grp")
    tile = lax.axis_index("tile")
    core = lax.rem(grp, 2)
    z_lo = grp // 2
    x = tile // 8
    z_hi = lax.rem(tile // 4, 2)
    y = lax.rem(tile, 4)
    z = z_hi * 2 + z_lo
    place = (x, y, z)
    sib, own, prt = (sib0, sib1), (own0, own1), (prt0, prt1)
    S = (s0, s1, s2)
    R = ((r10, r11, r12), (r20, r21, r22), (r30, r31, r32))
    T = ((t10, t11, t12), (t20, t21, t22))

    def peer(axis, d):
        to = [x, y, z]
        to[axis] = lax.rem(to[axis] + d, 4)
        px, py, pz = to
        return (lax.rem(pz, 2) * 2 + core, (px * 2 + pz // 2) * 4 + py)

    sibling = (z_lo * 2 + 1 - core, tile)

    barrier = pltpu.get_barrier_semaphore()
    pl.semaphore_signal(barrier, inc=1, device_id=sibling, device_id_type=MESH)
    for axis in range(3):
        for d in (1, 2, 3):
            pl.semaphore_signal(barrier, inc=1, device_id=peer(axis, d), device_id_type=MESH)

    def copy_a(k):
        return pltpu.make_async_copy(
            a_hbm.at[:, :, pl.ds(pl.multiple_of(k * KC, KC), KC)], a_raw.at[k], sem_a.at[k]
        )

    def copy_w(h, s, k):
        owner = core if s == 1 else 1 - core
        return pltpu.make_async_copy(
            w_hbm.at[:, owner, h, :, pl.ds(pl.multiple_of(k * KC, KC), KC)],
            wb.at[h, s, k],
            sem_w.at[h, s, k],
        )

    def start_first(k):
        copy_a(k).start()
        copy_w(0, 0, k).start()
        copy_w(0, 1, k).start()

    def wait_first(k):
        copy_a(k).wait()
        copy_w(0, 0, k).wait()
        copy_w(0, 1, k).wait()

    def prepare(k):
        first = (k * KC) // OCC
        lane = lax.broadcasted_iota(jnp.int32, (1, KC), 1)
        keep = [pm[jnp.minimum(first + j, 31)] for j in range(4)]
        edge = [OCC * (first + j + 1) - k * KC for j in range(3)]
        mask = jnp.where(
            lane < edge[0],
            keep[0],
            jnp.where(lane < edge[1], keep[1], jnp.where(lane < edge[2], keep[2], keep[3])),
        )
        mask = mask.astype(F32).astype(BF16)
        v = a_raw[k].reshape(32, 5, 4, KC)
        a2[k, 0:256] = v[:, 0:2].reshape(256, KC) * mask
        a2[k, 256:512] = v[:, 2:4].reshape(256, KC) * mask
        a2[k, 512:640] = v[:, 4].reshape(128, KC) * mask

    def product(h, s, k):
        return lax.dot_general(
            a2[k],
            wb[h, s, k].reshape(256, KC),
            (((1,), (1,)), ((), ())),
            preferred_element_type=F32,
        ).reshape(80, 8, 256)

    for k in range(AHEAD):
        start_first(k)

    wait_first(0)
    prepare(0)
    for ref in sib + own:
        ref[...] = jnp.zeros_like(ref)

    def step_first(k, carry):
        @pl.when(k + AHEAD < NK)
        def _():
            start_first(k + AHEAD)

        @pl.when(k + AHEAD >= NK)
        def _():
            for j in range(4):
                copy_w(1, 0, (k + AHEAD - NK) * 4 + j).start()

        wait_first(k + 1)
        prepare(k + 1)
        sib0[...] += product(0, 0, k)
        own0[...] += product(0, 1, k)
        return carry

    lax.fori_loop(0, NK - 1, step_first, 0)
    for k in range(12, NK):
        copy_w(1, 0, k).start()
    for k in range(NK):
        copy_w(1, 1, k).start()
    sib0[...] += product(0, 0, NK - 1)
    own0[...] += product(0, 1, NK - 1)

    pl.semaphore_wait(barrier, 10)

    def pair(h):
        return pltpu.make_async_remote_copy(
            src_ref=sib[h],
            dst_ref=prt[h],
            send_sem=dsend.at[h],
            recv_sem=drecv.at[h],
            device_id=sibling,
            device_id_type=MESH,
        )

    pair(0).start()

    def group(s, g):
        def step(k, carry):
            copy_w(1, s, k).wait()
            (sib1, own1)[s][...] += product(1, s, k)
            return carry

        lax.fori_loop(g * 5, g * 5 + 5, step, 0)

    def order(p):
        return [(p + j) % 3 for j in range(3)]

    def sems(h, p, stage, d):
        return ((h * 3 + p) * 3 + stage) * 3 + d - 1

    def send(h, p, stage, d):
        axis = order(p)[stage]
        there = lax.rem(place[axis] + d, 4)
        source = S[p].at[h, there] if stage == 0 else T[stage - 1][p].at[h, there]
        n = sems(h, p, stage, d)
        return pltpu.make_async_remote_copy(
            src_ref=source,
            dst_ref=R[stage][p].at[h, d - 1],
            send_sem=ssend.at[n],
            recv_sem=srecv.at[n],
            device_id=peer(axis, d),
            device_id_type=MESH,
        )

    def scatter(h):
        for p in range(3):
            for q in range(32):
                qx, qzh, qy = q // 8, (q // 4) % 2, q % 4
                o = om[q]
                for zl in range(2):
                    lanes = slice(zl * LANES, (zl + 1) * LANES)
                    if p < 2:
                        v = own[h][o + BASE[p], :, lanes] + prt[h][o + BASE[p], :, lanes]
                    else:
                        at = lax.shift_right_logical(o, 1) + BASE[p]
                        v = own[h][at, :, lanes] + prt[h][at, :, lanes]
                        odd = jnp.full((4, LANES), jnp.bitwise_and(o, 1))
                        v = jnp.where(odd == 1, v[4:8], v[0:4])
                    xyz = (qx, qy, qzh * 2 + zl)
                    i1, i2, i3 = (xyz[j] for j in order(p))
                    S[p][h, i1, i2, i3] = v
            for d in (2, 1, 3):
                send(h, p, 0, d).start()

    def collect(h, p, stage):
        axis = order(p)[stage]
        mine = S[p][h, place[axis]] if stage == 0 else T[stage - 1][p][h, place[axis]]
        for d in (1, 3, 2):
            send(h, p, stage, d).wait_recv()
        total = (mine + R[stage][p][h, 0]) + (R[stage][p][h, 1] + R[stage][p][h, 2])
        if stage < 2:
            T[stage][p][h] = total
            for d in (2, 1, 3):
                send(h, p, stage + 1, d).start()
        else:
            lanes = slice(h * LANES, (h + 1) * LANES)
            if p < 2:
                out[2 * p, :, lanes] = total[0:4]
                out[2 * p + 1, :, lanes] = total[4:8]
            else:
                out[4, :, lanes] = total

    group(0, 0)
    group(0, 1)
    group(0, 2)
    pair(1).start()
    pair(0).wait_recv()
    scatter(0)
    group(1, 0)
    group(1, 1)
    group(1, 2)
    pair(1).wait_recv()
    scatter(1)
    for stage in range(3):
        for h in range(2):
            for p in range(3):
                collect(h, p, stage)
    for h in range(2):
        pair(h).wait_send()
        for p in range(3):
            for stage in range(3):
                for d in (1, 2, 3):
                    send(h, p, stage, d).wait_send()


def local(amplitudes, w_vvvo, pair_mask, owner_map):
    w = w_vvvo.reshape(2, 2, 2, LANES, NK * KC)
    smem = pl.BlockSpec(memory_space=pltpu.SMEM)
    hbm = pl.BlockSpec(memory_space=pl.ANY)
    v = pltpu.VMEM
    scratch = [
        v((NK, 160, 4, KC), BF16),
        v((NK, 640, KC), BF16),
        v((2, 2, NK, 2, LANES, KC), BF16),
    ]
    scratch += [v((80, 8, 256), F32)] * 6
    scratch += [v((2, 4, 4, 4, r, LANES), F32) for r in ROWS]
    scratch += [v((2, 3, 4, 4, r, LANES), F32) for r in ROWS]
    scratch += [v((2, 3, 4, r, LANES), F32) for r in ROWS]
    scratch += [v((2, 3, r, LANES), F32) for r in ROWS]
    scratch += [v((2, 4, 4, r, LANES), F32) for r in ROWS]
    scratch += [v((2, 4, r, LANES), F32) for r in ROWS]
    scratch += [
        pltpu.SemaphoreType.DMA((NK,)),
        pltpu.SemaphoreType.DMA((2, 2, NK)),
        pltpu.SemaphoreType.DMA((2,)),
        pltpu.SemaphoreType.DMA((2,)),
        pltpu.SemaphoreType.DMA((54,)),
        pltpu.SemaphoreType.DMA((54,)),
    ]
    return pl.pallas_call(
        kernel,
        out_shape=jax.ShapeDtypeStruct((5, 4, 256), F32),
        in_specs=[smem, smem, hbm, hbm],
        out_specs=pl.BlockSpec(memory_space=pltpu.VMEM),
        scratch_shapes=scratch,
        compiler_params=pltpu.CompilerParams(
            collective_id=0, has_side_effects=True, vmem_limit_bytes=60 * 2**20
        ),
    )(pair_mask, owner_map, amplitudes, w)


def solution(mesh):
    return jax.shard_map(
        local,
        mesh=mesh,
        in_specs=(
            P(None, None, ("grp", "tile")),
            P(None, ("grp", "tile")),
            P(("grp", "tile")),
            P(),
        ),
        out_specs=P("tile", None, "grp"),
        check_vma=False,
    )
```

```python
import jax
import jax.numpy as jnp
from jax import lax
from jax.experimental import pallas as pl
from jax.experimental.pallas import tpu as pltpu
from jax.sharding import PartitionSpec as P

MESH = pl.DeviceIdType.MESH
F32 = jnp.float32
BF16 = jnp.bfloat16

KC = 512
GROUPS = (1, 2, 3, 4, 3, 2)
STARTS = tuple(sum(GROUPS[:j]) for j in range(len(GROUPS)))
SPLIT = 10
KT = 7680
OCC = 240
BASE = (0, 32, 64)
LANES = 128


def kernel(pm, om, a_hbm, w_hbm, out, *refs):
    n = len(GROUPS)
    a_raw, a2, w0, refs = refs[:n], refs[n : 2 * n], refs[2 * n : 3 * n], refs[3 * n :]
    w1, refs = refs[:3], refs[3:]
    sib, own, prt, refs = refs[:2], refs[2:4], refs[4:6], refs[6:]
    S, R, T, refs = refs[0], refs[1:4], refs[4:6], refs[6:]
    sem_a, sem_w, sem_w1, dsend, drecv, ssend, srecv = refs

    grp = lax.axis_index("grp")
    tile = lax.axis_index("tile")
    core = lax.rem(grp, 2)
    z_lo = grp // 2
    x = tile // 8
    z_hi = lax.rem(tile // 4, 2)
    y = lax.rem(tile, 4)
    place = (x, y, z_hi * 2 + z_lo)

    def peer(axis, d):
        to = list(place)
        to[axis] = lax.rem(to[axis] + d, 4)
        px, py, pz = to
        return (lax.rem(pz, 2) * 2 + core, (px * 2 + pz // 2) * 4 + py)

    sibling = (z_lo * 2 + 1 - core, tile)

    barrier = pltpu.get_barrier_semaphore()
    pl.semaphore_signal(barrier, inc=1, device_id=sibling, device_id_type=MESH)
    for axis in range(3):
        for d in (1, 2, 3):
            pl.semaphore_signal(barrier, inc=1, device_id=peer(axis, d), device_id_type=MESH)

    def columns(first, count):
        return pl.ds(first * KC, count * KC)

    def copies(g):
        cols = columns(STARTS[g], GROUPS[g])
        return (
            pltpu.make_async_copy(a_hbm.at[:, :, cols], a_raw[g], sem_a.at[g]),
            pltpu.make_async_copy(w_hbm.at[:, :, 0, :, cols], w0[g], sem_w.at[g]),
        )

    parts = ((1 - core, 0, SPLIT), (1 - core, SPLIT, 15 - SPLIT), (core, 0, 15))

    def late(j):
        who, first, count = parts[j]
        return pltpu.make_async_copy(
            w_hbm.at[:, who, 1, :, columns(first, count)], w1[j], sem_w1.at[j]
        )

    def prepare(g):
        masks = []
        for k in range(STARTS[g], STARTS[g] + GROUPS[g]):
            first = (k * KC) // OCC
            lane = lax.broadcasted_iota(jnp.int32, (1, KC), 1)
            keep = [pm[min(first + j, 31)] for j in range(4)]
            edge = [OCC * (first + j + 1) - k * KC for j in range(3)]
            row = jnp.where(lane < edge[2], keep[2], keep[3])
            row = jnp.where(lane < edge[0], keep[0], jnp.where(lane < edge[1], keep[1], row))
            masks.append(row.astype(F32).astype(BF16))
        width = GROUPS[g] * KC
        mask = jnp.concatenate(masks, axis=1)
        v = a_raw[g][...].reshape(32, 5, 4, width)
        a2[g][0:256] = v[:, 0:2].reshape(256, width) * mask
        a2[g][256:512] = v[:, 2:4].reshape(256, width) * mask
        a2[g][512:640] = v[:, 4].reshape(128, width) * mask

    def dot(a, w):
        return lax.dot_general(a, w, (((1,), (1,)), ((), ())), preferred_element_type=F32)

    def late_product(j):
        who, first, count = parts[j]
        total = None
        for g in range(n):
            lo, hi = max(first, STARTS[g]), min(first + count, STARTS[g] + GROUPS[g])
            if lo < hi:
                a = a2[g][:, (lo - STARTS[g]) * KC : (hi - STARTS[g]) * KC]
                w = w1[j][:, :, (lo - first) * KC : (hi - first) * KC].reshape(256, (hi - lo) * KC)
                d = dot(a, w)
                total = d if total is None else total + d
        return total.reshape(80, 8, 256)

    def pair(h):
        return pltpu.make_async_remote_copy(
            src_ref=sib[h],
            dst_ref=prt[h],
            send_sem=dsend.at[h],
            recv_sem=drecv.at[h],
            device_id=sibling,
            device_id_type=MESH,
        )

    def order(p):
        return [(p + j) % 3 for j in range(3)]

    def start_stage(h, stage, p):
        axis = order(p)[stage]
        for d in (2, 1, 3):
            there = lax.rem(place[axis] + d, 4)
            pltpu.make_async_remote_copy(
                src_ref=(S if stage == 0 else T[stage - 1]).at[h, p, there],
                dst_ref=R[stage].at[h, p, d - 1],
                send_sem=ssend.at[h * 3 + stage],
                recv_sem=srecv.at[h * 3 + stage],
                device_id=peer(axis, d),
                device_id_type=MESH,
            ).start()

    def whole_stage(h, stage):
        return pltpu.make_async_remote_copy(
            src_ref=R[stage].at[h],
            dst_ref=R[stage].at[h],
            send_sem=ssend.at[h * 3 + stage],
            recv_sem=srecv.at[h * 3 + stage],
            device_id=sibling,
            device_id_type=MESH,
        )

    def pair_sum(h, p):
        for q in range(32):
            qx, qzh, qy = q // 8, (q // 4) % 2, q % 4
            o = om[q]
            for zl in range(2):
                lanes = slice(zl * LANES, (zl + 1) * LANES)
                at = (o if p < 2 else lax.shift_right_logical(o, 1)) + BASE[p]
                v = own[h][at, :, lanes] + prt[h][at, :, lanes]
                if p == 2:
                    odd = jnp.full((8, LANES), jnp.bitwise_and(o, 1))
                    v = jnp.where(odd == 1, jnp.concatenate([v[4:8], v[0:4]], axis=0), v)
                xyz = (qx, qy, qzh * 2 + zl)
                i1, i2, i3 = (xyz[j] for j in order(p))
                S[h, p, i1, i2, i3] = v

    def collect(h, stage):
        whole_stage(h, stage).wait_recv()
        for p in range(3):
            mine = (S if stage == 0 else T[stage - 1])[h, p, place[order(p)[stage]]]
            r = R[stage]
            total = (mine + r[h, p, 0]) + (r[h, p, 1] + r[h, p, 2])
            if stage < 2:
                T[stage][h, p] = total
                start_stage(h, stage + 1, p)
            else:
                lanes = slice(h * LANES, (h + 1) * LANES)
                out[2 * p, :, lanes] = total[0:4]
                if p < 2:
                    out[2 * p + 1, :, lanes] = total[4:8]

    for g in range(n):
        for copy in copies(g):
            copy.start()
    for j in range(3):
        late(j).start()

    for g in range(n):
        for copy in copies(g):
            copy.wait()
        prepare(g)
        for ref, who in ((sib[0], 1 - core), (own[0], core)):
            w = w0[g][:, pl.ds(who, 1)].reshape(256, GROUPS[g] * KC)
            d = dot(a2[g][...], w).reshape(80, 8, 256)
            ref[...] = d if g == 0 else ref[...] + d

    pl.semaphore_wait(barrier, 10)
    pair(0).start()
    late(0).wait()
    sib[1][...] = late_product(0)
    late(1).wait()
    pair(0).wait_recv()
    for p in range(3):
        pair_sum(0, p)
    sib[1][...] += late_product(1)
    pair(1).start()
    for p in range(3):
        start_stage(0, 0, p)
    late(2).wait()
    own[1][...] = late_product(2)
    pair(1).wait_recv()
    for p in range(3):
        pair_sum(1, p)
        start_stage(1, 0, p)
    for stage in range(3):
        for h in range(2):
            collect(h, stage)
    for h in range(2):
        pair(h).wait_send()
        for stage in range(3):
            whole_stage(h, stage).wait_send()


def local(amplitudes, w_vvvo, pair_mask, owner_map):
    w = w_vvvo.reshape(2, 2, 2, LANES, KT)
    smem = pl.BlockSpec(memory_space=pltpu.SMEM)
    hbm = pl.BlockSpec(memory_space=pl.ANY)
    v = pltpu.VMEM
    dma = pltpu.SemaphoreType.DMA
    scratch = [v((160, 4, g * KC), BF16) for g in GROUPS]
    scratch += [v((640, g * KC), BF16) for g in GROUPS]
    scratch += [v((2, 2, LANES, g * KC), BF16) for g in GROUPS]
    scratch += [v((2, LANES, c * KC), BF16) for c in (SPLIT, 15 - SPLIT, 15)]
    scratch += [v((80, 8, 256), F32)] * 6
    scratch += [v((2, 3, 4, 4, 4, 8, LANES), F32)]
    scratch += [v((2, 3, 3, 4, 4, 8, LANES), F32), v((2, 3, 3, 4, 8, LANES), F32)]
    scratch += [v((2, 3, 3, 8, LANES), F32)]
    scratch += [v((2, 3, 4, 4, 8, LANES), F32), v((2, 3, 4, 8, LANES), F32)]
    scratch += [dma((len(GROUPS),)), dma((len(GROUPS),)), dma((3,)), dma((2,)), dma((2,)), dma((6,)), dma((6,))]
    return pl.pallas_call(
        kernel,
        out_shape=jax.ShapeDtypeStruct((5, 4, 256), F32),
        in_specs=[smem, smem, hbm, hbm],
        out_specs=pl.BlockSpec(memory_space=pltpu.VMEM),
        scratch_shapes=scratch,
        compiler_params=pltpu.CompilerParams(
            collective_id=0, has_side_effects=True, vmem_limit_bytes=62 * 2**20
        ),
    )(pair_mask, owner_map, amplitudes, w)


def solution(mesh):
    return jax.shard_map(
        local,
        mesh=mesh,
        in_specs=(
            P(None, None, ("grp", "tile")),
            P(None, ("grp", "tile")),
            P(("grp", "tile")),
            P(),
        ),
        out_specs=P("tile", None, "grp"),
        check_vma=False,
    )
```

```python
import jax
import jax.numpy as jnp
from jax import lax
from jax.experimental import pallas as pl
from jax.experimental.pallas import tpu as pltpu
from jax.sharding import PartitionSpec as P

MESH = pl.DeviceIdType.MESH
F32 = jnp.float32
BF16 = jnp.bfloat16

KC = 512
GROUPS = (1, 2, 3, 4, 3, 2)
STARTS = tuple(sum(GROUPS[:j]) for j in range(len(GROUPS)))
SPLIT = 12
KT = 7680
OCC = 240
BASE = (0, 32, 64)
LANES = 128


def kernel(pm_hbm, om_hbm, a_hbm, w_hbm, out, pm, om, *refs):
    n = len(GROUPS)
    a_raw, a2, w0, refs = refs[:n], refs[n : 2 * n], refs[2 * n : 3 * n], refs[3 * n :]
    w1, refs = refs[:3], refs[3:]
    sib, own, prt, refs = refs[:2], refs[2:4], refs[4:6], refs[6:]
    S, R, T, refs = refs[0], refs[1:4], refs[4:6], refs[6:]
    sem_m, sem_a, sem_w, sem_w1, dsend, drecv, ssend, srecv = refs

    grp = lax.axis_index("grp")
    tile = lax.axis_index("tile")
    core = lax.rem(grp, 2)
    z_lo = grp // 2
    x = tile // 8
    z_hi = lax.rem(tile // 4, 2)
    y = lax.rem(tile, 4)
    place = (x, y, z_hi * 2 + z_lo)

    def peer(axis, d):
        to = list(place)
        to[axis] = lax.rem(to[axis] + d, 4)
        px, py, pz = to
        return (lax.rem(pz, 2) * 2 + core, (px * 2 + pz // 2) * 4 + py)

    sibling = (z_lo * 2 + 1 - core, tile)

    def columns(first, count):
        return pl.ds(first * KC, count * KC)

    def copies(g):
        cols = columns(STARTS[g], GROUPS[g])
        return (
            pltpu.make_async_copy(a_hbm.at[:, :, cols], a_raw[g], sem_a.at[g]),
            pltpu.make_async_copy(w_hbm.at[:, :, 0, :, cols], w0[g], sem_w.at[g]),
        )

    parts = ((1 - core, 0, SPLIT), (1 - core, SPLIT, 15 - SPLIT), (core, 0, 15))

    def late(j):
        who, first, count = parts[j]
        return pltpu.make_async_copy(
            w_hbm.at[:, who, 1, :, columns(first, count)], w1[j], sem_w1.at[j]
        )

    def prepare(g):
        masks = []
        for k in range(STARTS[g], STARTS[g] + GROUPS[g]):
            first = (k * KC) // OCC
            lane = lax.broadcasted_iota(jnp.int32, (1, KC), 1)
            keep = [pm[min(first + j, 31)] for j in range(4)]
            edge = [OCC * (first + j + 1) - k * KC for j in range(3)]
            row = jnp.where(lane < edge[2], keep[2], keep[3])
            row = jnp.where(lane < edge[0], keep[0], jnp.where(lane < edge[1], keep[1], row))
            masks.append(row.astype(F32).astype(BF16))
        width = GROUPS[g] * KC
        mask = jnp.concatenate(masks, axis=1)
        v = a_raw[g][...].reshape(32, 5, 4, width)
        a2[g][0:256] = v[:, 0:2].reshape(256, width) * mask
        a2[g][256:512] = v[:, 2:4].reshape(256, width) * mask
        a2[g][512:640] = v[:, 4].reshape(128, width) * mask

    def dot(a, w):
        return lax.dot_general(a, w, (((1,), (1,)), ((), ())), preferred_element_type=F32)

    def late_product(j, top, bottom):
        who, first, count = parts[j]
        total = None
        for g in range(n):
            lo, hi = max(first, STARTS[g]), min(first + count, STARTS[g] + GROUPS[g])
            if lo < hi:
                a = a2[g][top:bottom, (lo - STARTS[g]) * KC : (hi - STARTS[g]) * KC]
                w = w1[j][:, :, (lo - first) * KC : (hi - first) * KC].reshape(256, (hi - lo) * KC)
                d = dot(a, w)
                total = d if total is None else total + d
        return total.reshape((bottom - top) // 8, 8, 256)

    def halves(ref, j, more):
        for top in (0, 320):
            rows = slice(top // 8, top // 8 + 40)
            d = late_product(j, top, top + 320)
            ref[rows] = ref[rows] + d if more else d

    def pair(h):
        return pltpu.make_async_remote_copy(
            src_ref=sib[h],
            dst_ref=prt[h],
            send_sem=dsend.at[h],
            recv_sem=drecv.at[h],
            device_id=sibling,
            device_id_type=MESH,
        )

    def order(p):
        return [(p + j) % 3 for j in range(3)]

    def start_stage(h, stage, p):
        axis = order(p)[stage]
        for d in (2, 1, 3):
            there = lax.rem(place[axis] + d, 4)
            pltpu.make_async_remote_copy(
                src_ref=(S if stage == 0 else T[stage - 1]).at[h, p, there],
                dst_ref=R[stage].at[h, p, d - 1],
                send_sem=ssend.at[h * 3 + stage],
                recv_sem=srecv.at[h * 3 + stage],
                device_id=peer(axis, d),
                device_id_type=MESH,
            ).start()

    def whole_stage(h, stage):
        return pltpu.make_async_remote_copy(
            src_ref=R[stage].at[h],
            dst_ref=R[stage].at[h],
            send_sem=ssend.at[h * 3 + stage],
            recv_sem=srecv.at[h * 3 + stage],
            device_id=sibling,
            device_id_type=MESH,
        )

    def pair_sum(h, p):
        for q in range(32):
            qx, qzh, qy = q // 8, (q // 4) % 2, q % 4
            o = om[q]
            for zl in range(2):
                lanes = slice(zl * LANES, (zl + 1) * LANES)
                at = (o if p < 2 else lax.shift_right_logical(o, 1)) + BASE[p]
                v = own[h][at, :, lanes] + prt[h][at, :, lanes]
                if p == 2:
                    odd = jnp.full((8, LANES), jnp.bitwise_and(o, 1))
                    v = jnp.where(odd == 1, jnp.concatenate([v[4:8], v[0:4]], axis=0), v)
                xyz = (qx, qy, qzh * 2 + zl)
                i1, i2, i3 = (xyz[j] for j in order(p))
                S[h, p, i1, i2, i3] = v

    def collect(h, stage):
        whole_stage(h, stage).wait_recv()
        for p in range(3):
            mine = (S if stage == 0 else T[stage - 1])[h, p, place[order(p)[stage]]]
            r = R[stage]
            total = (mine + r[h, p, 0]) + (r[h, p, 1] + r[h, p, 2])
            if stage < 2:
                T[stage][h, p] = total
                start_stage(h, stage + 1, p)
            else:
                lanes = slice(h * LANES, (h + 1) * LANES)
                out[2 * p, :, lanes] = total[0:4]
                if p < 2:
                    out[2 * p + 1, :, lanes] = total[4:8]

    tables = (
        pltpu.make_async_copy(pm_hbm, pm, sem_m.at[0]),
        pltpu.make_async_copy(om_hbm, om, sem_m.at[1]),
    )
    for copy in tables:
        copy.start()
    for g in range(n):
        for copy in copies(g):
            copy.start()
    for j in range(3):
        late(j).start()

    barrier = pltpu.get_barrier_semaphore()
    pl.semaphore_signal(barrier, inc=1, device_id=sibling, device_id_type=MESH)
    for axis in range(3):
        for d in (1, 2, 3):
            pl.semaphore_signal(barrier, inc=1, device_id=peer(axis, d), device_id_type=MESH)

    for copy in tables:
        copy.wait()

    for g in range(n):
        for copy in copies(g):
            copy.wait()
        prepare(g)
        for ref, who in ((sib[0], 1 - core), (own[0], core)):
            w = w0[g][:, pl.ds(who, 1)].reshape(256, GROUPS[g] * KC)
            d = dot(a2[g][...], w).reshape(80, 8, 256)
            ref[...] = d if g == 0 else ref[...] + d

    pl.semaphore_wait(barrier, 10)
    pair(0).start()
    late(0).wait()
    halves(sib[1], 0, False)
    late(1).wait()
    pair(0).wait_recv()
    for p in range(3):
        pair_sum(0, p)
    halves(sib[1], 1, True)
    pair(1).start()
    for p in range(3):
        start_stage(0, 0, p)
    late(2).wait()
    halves(own[1], 2, False)
    pair(1).wait_recv()
    for p in range(3):
        pair_sum(1, p)
        start_stage(1, 0, p)
    for stage in range(3):
        for h in range(2):
            collect(h, stage)
    for h in range(2):
        pair(h).wait_send()
        for stage in range(3):
            whole_stage(h, stage).wait_send()


def local(amplitudes, w_vvvo, pair_mask, owner_map):
    w = w_vvvo.reshape(2, 2, 2, LANES, KT)
    hbm = pl.BlockSpec(memory_space=pl.ANY)
    v = pltpu.VMEM
    dma = pltpu.SemaphoreType.DMA
    scratch = [pltpu.SMEM((32,), jnp.int32)] * 2
    scratch += [v((160, 4, g * KC), BF16) for g in GROUPS]
    scratch += [v((640, g * KC), BF16) for g in GROUPS]
    scratch += [v((2, 2, LANES, g * KC), BF16) for g in GROUPS]
    scratch += [v((2, LANES, c * KC), BF16) for c in (SPLIT, 15 - SPLIT, 15)]
    scratch += [v((80, 8, 256), F32)] * 6
    scratch += [v((2, 3, 4, 4, 4, 8, LANES), F32)]
    scratch += [v((2, 3, 3, 4, 4, 8, LANES), F32), v((2, 3, 3, 4, 8, LANES), F32)]
    scratch += [v((2, 3, 3, 8, LANES), F32)]
    scratch += [v((2, 3, 4, 4, 8, LANES), F32), v((2, 3, 4, 8, LANES), F32)]
    scratch += [dma((2,)), dma((len(GROUPS),)), dma((len(GROUPS),)), dma((3,)), dma((2,)), dma((2,)), dma((6,)), dma((6,))]
    return pl.pallas_call(
        kernel,
        out_shape=pltpu.VMEM((5, 4, 256), F32),
        in_specs=[hbm] * 4,
        out_specs=pl.BlockSpec(memory_space=pltpu.VMEM),
        scratch_shapes=scratch,
        compiler_params=pltpu.CompilerParams(
            collective_id=0, has_side_effects=True, vmem_limit_bytes=62 * 2**20
        ),
    )(pair_mask, owner_map, amplitudes, w)


def solution(mesh):
    return jax.shard_map(
        local,
        mesh=mesh,
        in_specs=(
            P(None, None, ("grp", "tile")),
            P(None, ("grp", "tile")),
            P(("grp", "tile")),
            P(),
        ),
        out_specs=P("tile", None, "grp"),
        check_vma=False,
    )
```

```python
import jax
import jax.numpy as jnp
from jax import lax
from jax.experimental import pallas as pl
from jax.experimental.pallas import tpu as pltpu
from jax.sharding import PartitionSpec as P

MESH = pl.DeviceIdType.MESH
F32 = jnp.float32
BF16 = jnp.bfloat16

KC = 512
GROUPS = (1, 2, 3, 4, 3, 2)
STARTS = tuple(sum(GROUPS[:j]) for j in range(len(GROUPS)))
SPLIT = 12
KT = 7680
OCC = 240
BASE = (0, 32, 64)
LANES = 128


def kernel(pm_hbm, om_hbm, a_hbm, w_hbm, out, pm, om, *refs):
    n = len(GROUPS)
    a_raw, a2, w0, refs = refs[:n], refs[n : 2 * n], refs[2 * n : 3 * n], refs[3 * n :]
    w1, refs = refs[:3], refs[3:]
    sib, own, prt, refs = refs[:2], refs[2:4], refs[4:6], refs[6:]
    S, R, T, plane, refs = refs[0], refs[1:4], refs[4:6], refs[6], refs[7:]
    sem_m, sem_a, sem_w, sem_w1, dsend, drecv, ssend, srecv = refs

    grp = lax.axis_index("grp")
    tile = lax.axis_index("tile")
    core = lax.rem(grp, 2)
    z_lo = grp // 2
    x = tile // 8
    z_hi = lax.rem(tile // 4, 2)
    y = lax.rem(tile, 4)
    place = (x, y, z_hi * 2 + z_lo)

    def peer(*moves):
        to = list(place)
        for axis, d in moves:
            to[axis] = lax.rem(to[axis] + d, 4)
        px, py, pz = to
        return (lax.rem(pz, 2) * 2 + core, (px * 2 + pz // 2) * 4 + py)

    sibling = (z_lo * 2 + 1 - core, tile)

    def columns(first, count):
        return pl.ds(first * KC, count * KC)

    def copies(g):
        cols = columns(STARTS[g], GROUPS[g])
        return (
            pltpu.make_async_copy(a_hbm.at[:, :, cols], a_raw[g], sem_a.at[g]),
            pltpu.make_async_copy(w_hbm.at[:, :, 0, :, cols], w0[g], sem_w.at[g]),
        )

    parts = ((1 - core, 0, SPLIT), (1 - core, SPLIT, 15 - SPLIT), (core, 0, 15))

    def late(j):
        who, first, count = parts[j]
        return pltpu.make_async_copy(
            w_hbm.at[:, who, 1, :, columns(first, count)], w1[j], sem_w1.at[j]
        )

    def prepare(g):
        masks = []
        for k in range(STARTS[g], STARTS[g] + GROUPS[g]):
            first = (k * KC) // OCC
            lane = lax.broadcasted_iota(jnp.int32, (1, KC), 1)
            keep = [pm[min(first + j, 31)] for j in range(4)]
            edge = [OCC * (first + j + 1) - k * KC for j in range(3)]
            row = jnp.where(lane < edge[2], keep[2], keep[3])
            row = jnp.where(lane < edge[0], keep[0], jnp.where(lane < edge[1], keep[1], row))
            masks.append(row.astype(F32).astype(BF16))
        width = GROUPS[g] * KC
        mask = jnp.concatenate(masks, axis=1)
        v = a_raw[g][...].reshape(32, 5, 4, width)
        a2[g][0:256] = v[:, 0:2].reshape(256, width) * mask
        a2[g][256:512] = v[:, 2:4].reshape(256, width) * mask
        a2[g][512:640] = v[:, 4].reshape(128, width) * mask

    def dot(a, w):
        return lax.dot_general(a, w, (((1,), (1,)), ((), ())), preferred_element_type=F32)

    def late_product(j, top, bottom):
        who, first, count = parts[j]
        total = None
        for g in range(n):
            lo, hi = max(first, STARTS[g]), min(first + count, STARTS[g] + GROUPS[g])
            if lo < hi:
                a = a2[g][top:bottom, (lo - STARTS[g]) * KC : (hi - STARTS[g]) * KC]
                w = w1[j][:, :, (lo - first) * KC : (hi - first) * KC].reshape(256, (hi - lo) * KC)
                d = dot(a, w)
                total = d if total is None else total + d
        return total.reshape((bottom - top) // 8, 8, 256)

    def halves(ref, j, more):
        for top in (0, 320):
            rows = slice(top // 8, top // 8 + 40)
            d = late_product(j, top, top + 320)
            ref[rows] = ref[rows] + d if more else d

    def pair(h):
        return pltpu.make_async_remote_copy(
            src_ref=sib[h],
            dst_ref=prt[h],
            send_sem=dsend.at[h],
            recv_sem=drecv.at[h],
            device_id=sibling,
            device_id_type=MESH,
        )

    def order(p):
        return [(p + j) % 3 for j in range(3)]

    def start_stage(h, stage, p):
        axis = order(p)[stage]
        for d in (2, 1, 3):
            there = lax.rem(place[axis] + d, 4)
            pltpu.make_async_remote_copy(
                src_ref=(S if stage == 0 else T[stage - 1]).at[h, p, there],
                dst_ref=R[stage].at[h, p, d - 1],
                send_sem=ssend.at[h * 3 + stage],
                recv_sem=srecv.at[h * 3 + stage],
                device_id=peer((axis, d)),
                device_id_type=MESH,
            ).start()

    def whole_stage(h, stage):
        return pltpu.make_async_remote_copy(
            src_ref=R[stage].at[h],
            dst_ref=R[stage].at[h],
            send_sem=ssend.at[h * 3 + stage],
            recv_sem=srecv.at[h * 3 + stage],
            device_id=sibling,
            device_id_type=MESH,
        )

    def pair_sum(h, p):
        for q in range(32):
            qx, qzh, qy = q // 8, (q // 4) % 2, q % 4
            o = om[q]
            for zl in range(2):
                lanes = slice(zl * LANES, (zl + 1) * LANES)
                at = (o if p < 2 else lax.shift_right_logical(o, 1)) + BASE[p]
                v = own[h][at, :, lanes] + prt[h][at, :, lanes]
                if p == 2:
                    odd = jnp.full((8, LANES), jnp.bitwise_and(o, 1))
                    v = jnp.where(odd == 1, jnp.concatenate([v[4:8], v[0:4]], axis=0), v)
                xyz = (qx, qy, qzh * 2 + zl)
                i1, i2, i3 = (xyz[j] for j in order(p))
                S[h, p, i1, i2, i3] = v

    def start_plane(p):
        _, b, c = order(p)
        for d in sorted(range(1, 16), key=lambda d: -(2 - abs(d // 4 - 2)) - (2 - abs(d % 4 - 2))):
            e, f = d // 4, d % 4
            source = T[0].at[1, p, lax.rem(place[b] + e, 4), lax.rem(place[c] + f, 4)]
            pltpu.make_async_remote_copy(
                src_ref=source,
                dst_ref=plane.at[p, d - 1],
                send_sem=ssend.at[4],
                recv_sem=srecv.at[4],
                device_id=peer(*[m for m in ((b, e), (c, f)) if m[1]]),
                device_id_type=MESH,
            ).start()

    def whole_plane():
        return pltpu.make_async_remote_copy(
            src_ref=plane,
            dst_ref=plane,
            send_sem=ssend.at[4],
            recv_sem=srecv.at[4],
            device_id=sibling,
            device_id_type=MESH,
        )

    def finish(h, p, total):
        lanes = slice(h * LANES, (h + 1) * LANES)
        out[2 * p, :, lanes] = total[0:4]
        if p < 2:
            out[2 * p + 1, :, lanes] = total[4:8]

    def collect_plane():
        whole_plane().wait_recv()
        for p in range(3):
            _, b, c = order(p)
            terms = [T[0][1, p, place[b], place[c]]] + [plane[p, j] for j in range(15)]
            while len(terms) > 1:
                terms = [u + w for u, w in zip(terms[::2], terms[1::2])]
            finish(1, p, terms[0])

    def collect(h, stage):
        whole_stage(h, stage).wait_recv()
        for p in range(3):
            mine = (S if stage == 0 else T[stage - 1])[h, p, place[order(p)[stage]]]
            r = R[stage]
            total = (mine + r[h, p, 0]) + (r[h, p, 1] + r[h, p, 2])
            if stage < 2:
                T[stage][h, p] = total
                if h == 0:
                    start_stage(h, stage + 1, p)
                else:
                    start_plane(p)
            else:
                finish(h, p, total)

    tables = (
        pltpu.make_async_copy(pm_hbm, pm, sem_m.at[0]),
        pltpu.make_async_copy(om_hbm, om, sem_m.at[1]),
    )
    for copy in tables:
        copy.start()
    for g in range(n):
        for copy in copies(g):
            copy.start()
    for j in range(3):
        late(j).start()

    barrier = pltpu.get_barrier_semaphore()
    pl.semaphore_signal(barrier, inc=1, device_id=sibling, device_id_type=MESH)
    for axis in range(3):
        for d in (1, 2, 3):
            for e in range(4):
                to = peer((axis, d), ((axis + 1) % 3, e)) if e else peer((axis, d))
                pl.semaphore_signal(barrier, inc=1, device_id=to, device_id_type=MESH)

    for copy in tables:
        copy.wait()

    for g in range(n):
        for copy in copies(g):
            copy.wait()
        prepare(g)
        for ref, who in ((sib[0], 1 - core), (own[0], core)):
            w = w0[g][:, pl.ds(who, 1)].reshape(256, GROUPS[g] * KC)
            d = dot(a2[g][...], w).reshape(80, 8, 256)
            ref[...] = d if g == 0 else ref[...] + d

    pl.semaphore_wait(barrier, 37)
    pair(0).start()
    late(0).wait()
    halves(sib[1], 0, False)
    late(1).wait()
    pair(0).wait_recv()
    for p in range(3):
        pair_sum(0, p)
    halves(sib[1], 1, True)
    pair(1).start()
    for p in range(3):
        start_stage(0, 0, p)
    late(2).wait()
    halves(own[1], 2, False)
    pair(1).wait_recv()
    for p in range(3):
        pair_sum(1, p)
        start_stage(1, 0, p)
    collect(0, 0)
    collect(1, 0)
    collect(0, 1)
    pair(0).wait_send()
    pair(1).wait_send()
    whole_stage(0, 0).wait_send()
    whole_stage(1, 0).wait_send()
    whole_stage(0, 1).wait_send()
    collect(0, 2)
    collect_plane()
    whole_stage(0, 2).wait_send()
    whole_plane().wait_send()


def local(amplitudes, w_vvvo, pair_mask, owner_map):
    w = w_vvvo.reshape(2, 2, 2, LANES, KT)
    hbm = pl.BlockSpec(memory_space=pl.ANY)
    v = pltpu.VMEM
    dma = pltpu.SemaphoreType.DMA
    scratch = [pltpu.SMEM((32,), jnp.int32)] * 2
    scratch += [v((160, 4, g * KC), BF16) for g in GROUPS]
    scratch += [v((640, g * KC), BF16) for g in GROUPS]
    scratch += [v((2, 2, LANES, g * KC), BF16) for g in GROUPS]
    scratch += [v((2, LANES, c * KC), BF16) for c in (SPLIT, 15 - SPLIT, 15)]
    scratch += [v((80, 8, 256), F32)] * 6
    scratch += [v((2, 3, 4, 4, 4, 8, LANES), F32)]
    scratch += [v((2, 3, 3, 4, 4, 8, LANES), F32), v((2, 3, 3, 4, 8, LANES), F32)]
    scratch += [v((2, 3, 3, 8, LANES), F32)]
    scratch += [v((2, 3, 4, 4, 8, LANES), F32), v((2, 3, 4, 8, LANES), F32)]
    scratch += [v((3, 15, 8, LANES), F32)]
    scratch += [dma((2,)), dma((len(GROUPS),)), dma((len(GROUPS),)), dma((3,)), dma((2,)), dma((2,)), dma((6,)), dma((6,))]
    return pl.pallas_call(
        kernel,
        out_shape=pltpu.VMEM((5, 4, 256), F32),
        in_specs=[hbm] * 4,
        out_specs=pl.BlockSpec(memory_space=pltpu.VMEM),
        scratch_shapes=scratch,
        compiler_params=pltpu.CompilerParams(
            collective_id=0, has_side_effects=True, vmem_limit_bytes=62 * 2**20
        ),
    )(pair_mask, owner_map, amplitudes, w)


def solution(mesh):
    return jax.shard_map(
        local,
        mesh=mesh,
        in_specs=(
            P(None, None, ("grp", "tile")),
            P(None, ("grp", "tile")),
            P(("grp", "tile")),
            P(),
        ),
        out_specs=P("tile", None, "grp"),
        check_vma=False,
    )
```

```python
import jax
import jax.numpy as jnp
from jax import lax
from jax.experimental import pallas as pl
from jax.experimental.pallas import tpu as pltpu
from jax.sharding import PartitionSpec as P

MESH = pl.DeviceIdType.MESH
F32 = jnp.float32
BF16 = jnp.bfloat16

KC = 512
GROUPS = (1, 1, 2, 2, 3, 3, 2, 1)
STARTS = tuple(sum(GROUPS[:j]) for j in range(len(GROUPS)))
SPLIT = 12
KT = 7680
OCC = 240
BASE = (0, 32, 64)
LANES = 128


def kernel(pm_hbm, om_hbm, a_hbm, w_hbm, out, pm, om, *refs):
    n = len(GROUPS)
    a_raw, a2, w0, refs = refs[:n], refs[n : 2 * n], refs[2 * n : 3 * n], refs[3 * n :]
    w1, refs = refs[:3], refs[3:]
    sib, own, prt, refs = refs[:2], refs[2:4], refs[4:6], refs[6:]
    S, R, T, plane, refs = refs[0], refs[1:4], refs[4:6], refs[6], refs[7:]
    sem_m, sem_a, sem_w, sem_w1, dsend, drecv, ssend, srecv = refs

    grp = lax.axis_index("grp")
    tile = lax.axis_index("tile")
    core = lax.rem(grp, 2)
    z_lo = grp // 2
    x = tile // 8
    z_hi = lax.rem(tile // 4, 2)
    y = lax.rem(tile, 4)
    place = (x, y, z_hi * 2 + z_lo)

    def peer(*moves):
        to = list(place)
        for axis, d in moves:
            to[axis] = lax.rem(to[axis] + d, 4)
        px, py, pz = to
        return (lax.rem(pz, 2) * 2 + core, (px * 2 + pz // 2) * 4 + py)

    sibling = (z_lo * 2 + 1 - core, tile)

    def columns(first, count):
        return pl.ds(first * KC, count * KC)

    def copies(g):
        cols = columns(STARTS[g], GROUPS[g])
        return (
            pltpu.make_async_copy(a_hbm.at[:, :, cols], a_raw[g], sem_a.at[g]),
            pltpu.make_async_copy(w_hbm.at[:, :, 0, :, cols], w0[g], sem_w.at[g]),
        )

    parts = ((1 - core, 0, SPLIT), (1 - core, SPLIT, 15 - SPLIT), (core, 0, 15))

    def late(j):
        who, first, count = parts[j]
        return pltpu.make_async_copy(
            w_hbm.at[:, who, 1, :, columns(first, count)], w1[j], sem_w1.at[j]
        )

    def prepare(g):
        masks = []
        for k in range(STARTS[g], STARTS[g] + GROUPS[g]):
            first = (k * KC) // OCC
            lane = lax.broadcasted_iota(jnp.int32, (1, KC), 1)
            keep = [pm[min(first + j, 31)] for j in range(4)]
            edge = [OCC * (first + j + 1) - k * KC for j in range(3)]
            row = jnp.where(lane < edge[2], keep[2], keep[3])
            row = jnp.where(lane < edge[0], keep[0], jnp.where(lane < edge[1], keep[1], row))
            masks.append(row.astype(F32).astype(BF16))
        width = GROUPS[g] * KC
        mask = jnp.concatenate(masks, axis=1)
        v = a_raw[g][...].reshape(32, 5, 4, width)
        a2[g][0:256] = v[:, 0:2].reshape(256, width) * mask
        a2[g][256:512] = v[:, 2:4].reshape(256, width) * mask
        a2[g][512:640] = v[:, 4].reshape(128, width) * mask

    def dot(a, w):
        return lax.dot_general(a, w, (((1,), (1,)), ((), ())), preferred_element_type=F32)

    def late_product(j, top, bottom):
        who, first, count = parts[j]
        total = None
        for g in range(n):
            lo, hi = max(first, STARTS[g]), min(first + count, STARTS[g] + GROUPS[g])
            if lo < hi:
                a = a2[g][top:bottom, (lo - STARTS[g]) * KC : (hi - STARTS[g]) * KC]
                w = w1[j][:, :, (lo - first) * KC : (hi - first) * KC].reshape(256, (hi - lo) * KC)
                d = dot(a, w)
                total = d if total is None else total + d
        return total.reshape((bottom - top) // 8, 8, 256)

    def halves(ref, j, more):
        for top in (0, 320):
            rows = slice(top // 8, top // 8 + 40)
            d = late_product(j, top, top + 320)
            ref[rows] = ref[rows] + d if more else d

    def pair(h):
        return pltpu.make_async_remote_copy(
            src_ref=sib[h],
            dst_ref=prt[h],
            send_sem=dsend.at[h],
            recv_sem=drecv.at[h],
            device_id=sibling,
            device_id_type=MESH,
        )

    def order(p):
        return [(p + j) % 3 for j in range(3)]

    def start_stage(h, stage, p):
        axis = order(p)[stage]
        for d in (2, 1, 3):
            there = lax.rem(place[axis] + d, 4)
            pltpu.make_async_remote_copy(
                src_ref=(S if stage == 0 else T[stage - 1]).at[h, p, there],
                dst_ref=R[stage].at[h, p, d - 1],
                send_sem=ssend.at[h * 9 + stage * 3 + p],
                recv_sem=srecv.at[h * 9 + stage * 3 + p],
                device_id=peer((axis, d)),
                device_id_type=MESH,
            ).start()

    def whole_stage(h, stage, p):
        return pltpu.make_async_remote_copy(
            src_ref=R[stage].at[h, p],
            dst_ref=R[stage].at[h, p],
            send_sem=ssend.at[h * 9 + stage * 3 + p],
            recv_sem=srecv.at[h * 9 + stage * 3 + p],
            device_id=sibling,
            device_id_type=MESH,
        )

    def pair_sum(h, p):
        for q in range(32):
            qx, qzh, qy = q // 8, (q // 4) % 2, q % 4
            o = om[q]
            for zl in range(2):
                lanes = slice(zl * LANES, (zl + 1) * LANES)
                at = (o if p < 2 else lax.shift_right_logical(o, 1)) + BASE[p]
                v = own[h][at, :, lanes] + prt[h][at, :, lanes]
                if p == 2:
                    odd = jnp.full((8, LANES), jnp.bitwise_and(o, 1))
                    v = jnp.where(odd == 1, jnp.concatenate([v[4:8], v[0:4]], axis=0), v)
                xyz = (qx, qy, qzh * 2 + zl)
                i1, i2, i3 = (xyz[j] for j in order(p))
                S[h, p, i1, i2, i3] = v

    def start_plane(p):
        _, b, c = order(p)
        for d in sorted(range(1, 16), key=lambda d: -(2 - abs(d // 4 - 2)) - (2 - abs(d % 4 - 2))):
            e, f = d // 4, d % 4
            source = T[0].at[1, p, lax.rem(place[b] + e, 4), lax.rem(place[c] + f, 4)]
            pltpu.make_async_remote_copy(
                src_ref=source,
                dst_ref=plane.at[p, d - 1],
                send_sem=ssend.at[12 + p],
                recv_sem=srecv.at[12 + p],
                device_id=peer(*[m for m in ((b, e), (c, f)) if m[1]]),
                device_id_type=MESH,
            ).start()

    def whole_plane(p):
        return pltpu.make_async_remote_copy(
            src_ref=plane.at[p],
            dst_ref=plane.at[p],
            send_sem=ssend.at[12 + p],
            recv_sem=srecv.at[12 + p],
            device_id=sibling,
            device_id_type=MESH,
        )

    def finish(h, p, total):
        lanes = slice(h * LANES, (h + 1) * LANES)
        out[2 * p, :, lanes] = total[0:4]
        if p < 2:
            out[2 * p + 1, :, lanes] = total[4:8]

    def collect_plane():
        for p in range(3):
            whole_plane(p).wait_recv()
            _, b, c = order(p)
            terms = [T[0][1, p, place[b], place[c]]] + [plane[p, j] for j in range(15)]
            while len(terms) > 1:
                terms = [u + w for u, w in zip(terms[::2], terms[1::2])]
            finish(1, p, terms[0])

    def collect(h, stage):
        for p in range(3):
            whole_stage(h, stage, p).wait_recv()
            mine = (S if stage == 0 else T[stage - 1])[h, p, place[order(p)[stage]]]
            r = R[stage]
            total = (mine + r[h, p, 0]) + (r[h, p, 1] + r[h, p, 2])
            if stage < 2:
                T[stage][h, p] = total
                if h == 0:
                    start_stage(h, stage + 1, p)
                else:
                    start_plane(p)
            else:
                finish(h, p, total)

    tables = (
        pltpu.make_async_copy(pm_hbm, pm, sem_m.at[0]),
        pltpu.make_async_copy(om_hbm, om, sem_m.at[1]),
    )
    for copy in tables:
        copy.start()
    for g in range(n):
        for copy in copies(g):
            copy.start()
    for j in range(3):
        late(j).start()

    barrier = pltpu.get_barrier_semaphore()
    pl.semaphore_signal(barrier, inc=1, device_id=sibling, device_id_type=MESH)
    for axis in range(3):
        for d in (1, 2, 3):
            for e in range(4):
                to = peer((axis, d), ((axis + 1) % 3, e)) if e else peer((axis, d))
                pl.semaphore_signal(barrier, inc=1, device_id=to, device_id_type=MESH)

    for copy in tables:
        copy.wait()

    for g in range(n):
        for copy in copies(g):
            copy.wait()
        prepare(g)
        for ref, who in ((sib[0], 1 - core), (own[0], core)):
            w = w0[g][:, pl.ds(who, 1)].reshape(256, GROUPS[g] * KC)
            d = dot(a2[g][...], w).reshape(80, 8, 256)
            ref[...] = d if g == 0 else ref[...] + d

    pl.semaphore_wait(barrier, 37)
    pair(0).start()
    late(0).wait()
    halves(sib[1], 0, False)
    late(1).wait()
    pair(0).wait_recv()
    for p in range(3):
        pair_sum(0, p)
    halves(sib[1], 1, True)
    pair(1).start()
    for p in range(3):
        start_stage(0, 0, p)
    late(2).wait()
    halves(own[1], 2, False)
    pair(1).wait_recv()
    for p in range(3):
        pair_sum(1, p)
        start_stage(1, 0, p)
    collect(0, 0)
    collect(1, 0)
    collect(0, 1)
    pair(0).wait_send()
    pair(1).wait_send()
    for h, stage in ((0, 0), (1, 0), (0, 1)):
        for p in range(3):
            whole_stage(h, stage, p).wait_send()
    collect(0, 2)
    collect_plane()
    for p in range(3):
        whole_stage(0, 2, p).wait_send()
        whole_plane(p).wait_send()


def local(amplitudes, w_vvvo, pair_mask, owner_map):
    w = w_vvvo.reshape(2, 2, 2, LANES, KT)
    hbm = pl.BlockSpec(memory_space=pl.ANY)
    v = pltpu.VMEM
    dma = pltpu.SemaphoreType.DMA
    scratch = [pltpu.SMEM((32,), jnp.int32)] * 2
    scratch += [v((160, 4, g * KC), BF16) for g in GROUPS]
    scratch += [v((640, g * KC), BF16) for g in GROUPS]
    scratch += [v((2, 2, LANES, g * KC), BF16) for g in GROUPS]
    scratch += [v((2, LANES, c * KC), BF16) for c in (SPLIT, 15 - SPLIT, 15)]
    scratch += [v((80, 8, 256), F32)] * 6
    scratch += [v((2, 3, 4, 4, 4, 8, LANES), F32)]
    scratch += [v((2, 3, 3, 4, 4, 8, LANES), F32), v((2, 3, 3, 4, 8, LANES), F32)]
    scratch += [v((2, 3, 3, 8, LANES), F32)]
    scratch += [v((2, 3, 4, 4, 8, LANES), F32), v((2, 3, 4, 8, LANES), F32)]
    scratch += [v((3, 15, 8, LANES), F32)]
    scratch += [dma((2,)), dma((len(GROUPS),)), dma((len(GROUPS),)), dma((3,)), dma((2,)), dma((2,)), dma((18,)), dma((18,))]
    return pl.pallas_call(
        kernel,
        out_shape=pltpu.VMEM((5, 4, 256), F32),
        in_specs=[hbm] * 4,
        out_specs=pl.BlockSpec(memory_space=pltpu.VMEM),
        scratch_shapes=scratch,
        compiler_params=pltpu.CompilerParams(
            collective_id=0, has_side_effects=True, vmem_limit_bytes=62 * 2**20
        ),
    )(pair_mask, owner_map, amplitudes, w)


def solution(mesh):
    return jax.shard_map(
        local,
        mesh=mesh,
        in_specs=(
            P(None, None, ("grp", "tile")),
            P(None, ("grp", "tile")),
            P(("grp", "tile")),
            P(),
        ),
        out_specs=P("tile", None, "grp"),
        check_vma=False,
    )
```

```python
import jax
import jax.numpy as jnp
from jax import lax
from jax.experimental import pallas as pl
from jax.experimental.pallas import tpu as pltpu
from jax.sharding import PartitionSpec as P

MESH = pl.DeviceIdType.MESH
F32 = jnp.float32
BF16 = jnp.bfloat16

KC = 512
GROUPS = (1, 1, 2, 2, 3, 3, 2, 1)
STARTS = tuple(sum(GROUPS[:j]) for j in range(len(GROUPS)))
SPLIT = 12
KT = 7680
OCC = 240
BASE = (0, 32, 64)
LANES = 128


def kernel(pm_hbm, om_hbm, a_hbm, w_hbm, out, pm, om, *refs):
    n = len(GROUPS)
    a_raw, a2, w0, refs = refs[:n], refs[n : 2 * n], refs[2 * n : 3 * n], refs[3 * n :]
    w1, refs = refs[:3], refs[3:]
    sib, own, prt, refs = refs[:2], refs[2:4], refs[4:6], refs[6:]
    S, R, T, plane, refs = refs[0], refs[1:4], refs[4:6], refs[6], refs[7:]
    sem_m, sem_a, sem_w, sem_w1, dsend, drecv, ssend, srecv = refs

    grp = lax.axis_index("grp")
    tile = lax.axis_index("tile")
    core = lax.rem(grp, 2)
    z_lo = grp // 2
    x = tile // 8
    z_hi = lax.rem(tile // 4, 2)
    y = lax.rem(tile, 4)
    place = (x, y, z_hi * 2 + z_lo)

    def peer(*moves):
        to = list(place)
        for axis, d in moves:
            to[axis] = lax.rem(to[axis] + d, 4)
        px, py, pz = to
        return (lax.rem(pz, 2) * 2 + core, (px * 2 + pz // 2) * 4 + py)

    sibling = (z_lo * 2 + 1 - core, tile)

    def columns(first, count):
        return pl.ds(first * KC, count * KC)

    def copies(g):
        cols = columns(STARTS[g], GROUPS[g])
        return (
            pltpu.make_async_copy(a_hbm.at[:, :, cols], a_raw[g], sem_a.at[g]),
            pltpu.make_async_copy(w_hbm.at[:, :, 0, :, cols], w0[g], sem_w.at[g]),
        )

    parts = ((1 - core, 0, SPLIT), (1 - core, SPLIT, 15 - SPLIT), (core, 0, 15))

    def late(j):
        who, first, count = parts[j]
        return pltpu.make_async_copy(
            w_hbm.at[:, who, 1, :, columns(first, count)], w1[j], sem_w1.at[j]
        )

    def prepare(g):
        masks = []
        for k in range(STARTS[g], STARTS[g] + GROUPS[g]):
            first = (k * KC) // OCC
            lane = lax.broadcasted_iota(jnp.int32, (1, KC), 1)
            keep = [pm[min(first + j, 31)] for j in range(4)]
            edge = [OCC * (first + j + 1) - k * KC for j in range(3)]
            row = jnp.where(lane < edge[2], keep[2], keep[3])
            row = jnp.where(lane < edge[0], keep[0], jnp.where(lane < edge[1], keep[1], row))
            masks.append(row.astype(F32).astype(BF16))
        width = GROUPS[g] * KC
        mask = jnp.concatenate(masks, axis=1)
        v = a_raw[g][...].reshape(32, 5, 4, width)
        a2[g][0:256] = v[:, 0:2].reshape(256, width) * mask
        a2[g][256:512] = v[:, 2:4].reshape(256, width) * mask
        a2[g][512:640] = v[:, 4].reshape(128, width) * mask

    def dot(a, w):
        return lax.dot_general(a, w, (((1,), (1,)), ((), ())), preferred_element_type=F32)

    def late_product(j, top, bottom):
        who, first, count = parts[j]
        total = None
        for g in range(n):
            lo, hi = max(first, STARTS[g]), min(first + count, STARTS[g] + GROUPS[g])
            if lo < hi:
                a = a2[g][top:bottom, (lo - STARTS[g]) * KC : (hi - STARTS[g]) * KC]
                w = w1[j][:, :, (lo - first) * KC : (hi - first) * KC].reshape(256, (hi - lo) * KC)
                d = dot(a, w)
                total = d if total is None else total + d
        return total.reshape((bottom - top) // 8, 8, 256)

    def halves(ref, j, more):
        for top in (0, 320):
            rows = slice(top // 8, top // 8 + 40)
            d = late_product(j, top, top + 320)
            ref[rows] = ref[rows] + d if more else d

    def pair(h):
        return pltpu.make_async_remote_copy(
            src_ref=sib[h],
            dst_ref=prt[h],
            send_sem=dsend.at[h],
            recv_sem=drecv.at[h],
            device_id=sibling,
            device_id_type=MESH,
        )

    def order(p):
        return [(p + j) % 3 for j in range(3)]

    def start_stage(h, stage, p):
        axis = order(p)[stage]
        for d in (2, 1, 3):
            there = lax.rem(place[axis] + d, 4)
            pltpu.make_async_remote_copy(
                src_ref=(S if stage == 0 else T[stage - 1]).at[h, p, there],
                dst_ref=R[stage].at[h, p, d - 1],
                send_sem=ssend.at[h * 9 + stage * 3 + p],
                recv_sem=srecv.at[h * 9 + stage * 3 + p],
                device_id=peer((axis, d)),
                device_id_type=MESH,
            ).start()

    def whole_stage(h, stage, p):
        return pltpu.make_async_remote_copy(
            src_ref=R[stage].at[h, p],
            dst_ref=R[stage].at[h, p],
            send_sem=ssend.at[h * 9 + stage * 3 + p],
            recv_sem=srecv.at[h * 9 + stage * 3 + p],
            device_id=sibling,
            device_id_type=MESH,
        )

    def pair_sum(h, p):
        for q in range(32):
            qx, qzh, qy = q // 8, (q // 4) % 2, q % 4
            o = om[q]
            for zl in range(2):
                lanes = slice(zl * LANES, (zl + 1) * LANES)
                at = (o if p < 2 else lax.shift_right_logical(o, 1)) + BASE[p]
                v = own[h][at, :, lanes] + prt[h][at, :, lanes]
                if p == 2:
                    odd = jnp.full((8, LANES), jnp.bitwise_and(o, 1))
                    v = jnp.where(odd == 1, jnp.concatenate([v[4:8], v[0:4]], axis=0), v)
                xyz = (qx, qy, qzh * 2 + zl)
                i1, i2, i3 = (xyz[j] for j in order(p))
                S[h, p, i1, i2, i3] = v

    def start_plane(p):
        _, b, c = order(p)
        for d in sorted(range(1, 16), key=lambda d: -(2 - abs(d // 4 - 2)) - (2 - abs(d % 4 - 2))):
            e, f = d // 4, d % 4
            source = T[0].at[1, p, lax.rem(place[b] + e, 4), lax.rem(place[c] + f, 4)]
            pltpu.make_async_remote_copy(
                src_ref=source,
                dst_ref=plane.at[p, d - 1],
                send_sem=ssend.at[12 + p],
                recv_sem=srecv.at[12 + p],
                device_id=peer(*[m for m in ((b, e), (c, f)) if m[1]]),
                device_id_type=MESH,
            ).start()

    def whole_plane(p):
        return pltpu.make_async_remote_copy(
            src_ref=plane.at[p],
            dst_ref=plane.at[p],
            send_sem=ssend.at[12 + p],
            recv_sem=srecv.at[12 + p],
            device_id=sibling,
            device_id_type=MESH,
        )

    def finish(h, p, total):
        lanes = slice(h * LANES, (h + 1) * LANES)
        out[2 * p, :, lanes] = total[0:4]
        if p < 2:
            out[2 * p + 1, :, lanes] = total[4:8]

    def collect_plane():
        for p in range(3):
            whole_plane(p).wait_recv()
            _, b, c = order(p)
            terms = [T[0][1, p, place[b], place[c]]] + [plane[p, j] for j in range(15)]
            while len(terms) > 1:
                terms = [u + w for u, w in zip(terms[::2], terms[1::2])]
            finish(1, p, terms[0])

    def collect(h, stage):
        for p in range(3):
            whole_stage(h, stage, p).wait_recv()
            mine = (S if stage == 0 else T[stage - 1])[h, p, place[order(p)[stage]]]
            r = R[stage]
            total = (mine + r[h, p, 0]) + (r[h, p, 1] + r[h, p, 2])
            if stage < 2:
                T[stage][h, p] = total
                if h == 0:
                    start_stage(h, stage + 1, p)
                else:
                    start_plane(p)
            else:
                finish(h, p, total)

    tables = (
        pltpu.make_async_copy(pm_hbm, pm, sem_m.at[0]),
        pltpu.make_async_copy(om_hbm, om, sem_m.at[1]),
    )
    for copy in tables:
        copy.start()
    for g in range(n):
        for copy in copies(g):
            copy.start()
    for j in range(3):
        late(j).start()

    barrier = pltpu.get_barrier_semaphore()
    pl.semaphore_signal(barrier, inc=1, device_id=sibling, device_id_type=MESH)
    for axis in range(3):
        for d in (1, 2, 3):
            for e in range(4):
                to = peer((axis, d), ((axis + 1) % 3, e)) if e else peer((axis, d))
                pl.semaphore_signal(barrier, inc=1, device_id=to, device_id_type=MESH)

    for copy in tables:
        copy.wait()

    for g in range(n):
        for copy in copies(g):
            copy.wait()
        prepare(g)
        for ref, who in ((sib[0], 1 - core), (own[0], core)):
            w = w0[g][:, pl.ds(who, 1)].reshape(256, GROUPS[g] * KC)
            d = dot(a2[g][...], w).reshape(80, 8, 256)
            ref[...] = d if g == 0 else ref[...] + d

    pl.semaphore_wait(barrier, 37)
    pair(0).start()
    late(0).wait()
    halves(sib[1], 0, False)
    late(1).wait()
    pair(0).wait_recv()
    for p in range(3):
        pair_sum(0, p)
    halves(sib[1], 1, True)
    pair(1).start()
    for p in range(3):
        start_stage(0, 0, p)
    late(2).wait()
    halves(own[1], 2, False)
    pair(1).wait_recv()
    for p in range(3):
        pair_sum(1, p)
        start_stage(1, 0, p)
    collect(0, 0)
    collect(1, 0)
    collect(0, 1)
    pair(0).wait_send()
    pair(1).wait_send()
    for h, stage in ((0, 0), (1, 0), (0, 1)):
        for p in range(3):
            whole_stage(h, stage, p).wait_send()
    collect_plane()
    collect(0, 2)
    for p in range(3):
        whole_stage(0, 2, p).wait_send()
        whole_plane(p).wait_send()


def local(amplitudes, w_vvvo, pair_mask, owner_map):
    w = w_vvvo.reshape(2, 2, 2, LANES, KT)
    hbm = pl.BlockSpec(memory_space=pl.ANY)
    v = pltpu.VMEM
    dma = pltpu.SemaphoreType.DMA
    scratch = [pltpu.SMEM((32,), jnp.int32)] * 2
    scratch += [v((160, 4, g * KC), BF16) for g in GROUPS]
    scratch += [v((640, g * KC), BF16) for g in GROUPS]
    scratch += [v((2, 2, LANES, g * KC), BF16) for g in GROUPS]
    scratch += [v((2, LANES, c * KC), BF16) for c in (SPLIT, 15 - SPLIT, 15)]
    scratch += [v((80, 8, 256), F32)] * 6
    scratch += [v((2, 3, 4, 4, 4, 8, LANES), F32)]
    scratch += [v((2, 3, 3, 4, 4, 8, LANES), F32), v((2, 3, 3, 4, 8, LANES), F32)]
    scratch += [v((2, 3, 3, 8, LANES), F32)]
    scratch += [v((2, 3, 4, 4, 8, LANES), F32), v((2, 3, 4, 8, LANES), F32)]
    scratch += [v((3, 15, 8, LANES), F32)]
    scratch += [dma((2,)), dma((len(GROUPS),)), dma((len(GROUPS),)), dma((3,)), dma((2,)), dma((2,)), dma((18,)), dma((18,))]
    return pl.pallas_call(
        kernel,
        out_shape=pltpu.VMEM((5, 4, 256), F32),
        in_specs=[hbm] * 4,
        out_specs=pl.BlockSpec(memory_space=pltpu.VMEM),
        scratch_shapes=scratch,
        compiler_params=pltpu.CompilerParams(
            collective_id=0, has_side_effects=True, vmem_limit_bytes=62 * 2**20
        ),
    )(pair_mask, owner_map, amplitudes, w)


def solution(mesh):
    return jax.shard_map(
        local,
        mesh=mesh,
        in_specs=(
            P(None, None, ("grp", "tile")),
            P(None, ("grp", "tile")),
            P(("grp", "tile")),
            P(),
        ),
        out_specs=P("tile", None, "grp"),
        check_vma=False,
    )
```
